512 devices in a mesh: aux: 32 (over y, x, core), shell: 16 (over z).
Axes of the slice: x: 4, y: 4, z: 16, core: 2. Of those that a mesh axis runs over, the one named last changes fastest.
Arguments:
- density: bfloat16 [128, 120, 8192], P('aux', None, 'shell'), may hold values from -6 to 6
- occ_density: bfloat16 [128, 120, 120], P('aux'), may hold values from -6 to 6
- cabs_coeff: bfloat16 [2048, 8192], P('aux', 'shell'), may hold values from -0.0625 to 0.0625
- occ_coeff: bfloat16 [2048, 120], P('aux'), may hold values from -0.5 to 0.5
- tile_owner: int32 [64, 1], replicated, may hold values from 0 to 15; in each aligned block of 64 rows (0 to 63, 64 to 127, ...) at most 8 rows name the same one
Outputs:
- ao_density: bfloat16 [128, 128, 32, 2048], P('shell', 'aux')
The draws below stay inside these ranges and needn't reach their ends.
Inputs may be any that keep to these rules, and one draw needn't show every extreme that they name: `tile_owner`: no owner holds more than 8 blocks, and some owner holds exactly 8; every owner holds at least one block.
All inputs are finite; a program needn't handle non-finite values.
Results may differ from the reference program's by a relative error of at most 0.015.
Values may be sent and summed in bfloat16 or wider, within the bound.
A program may use at most 64 MiB of HBM per device.

```python
import math
import jax
import jax.numpy as jnp
import numpy as np
from jax import lax

NOCC = 120
NAO = 2048
NCABS = 8192
CAPT = 8
NTILE = 64
BW = 32
NAUX = 128
N_SHELL = 16


def level_of(rng, extent, shards, low, high):
    loudness = 1.0
    for dim, parts in shards:
        draws = jax.random.uniform(jax.random.fold_in(jax.random.fold_in(rng, 6), dim), (parts,), jnp.float32, low / len(shards), high / len(shards))
        loudness = loudness * jnp.repeat(jnp.exp(draws), extent[dim] // parts).reshape((-1,) + (1,) * (len(extent) - 1 - dim))
    return loudness


def shared_out(own_key, own, number, rows, number_of, top, limit, skew):
    ranking = jax.random.permutation(own_key, number_of)
    packed, common = portions_of(number_of, rows * top, limit, skew, True), portions_of(number_of, rows * top, limit, skew, False)
    places = jnp.arange(number_of)

    def named(tallies, offset_by):
        used = int((tallies > 0).sum())
        fixed = max(1, used // 4)
        passed = fixed + (places - fixed + offset_by * (used - fixed)) % max(1, number_of - fixed)
        return jnp.zeros((number_of,), jnp.int32).at[ranking[jnp.where(places < fixed, places, passed)]].set(jnp.asarray(tallies, jnp.int32))

    tallies = jnp.where(number % 4 == 0, named(packed, number // 4), named(common, number - number // 4 - 1))
    mixed = jax.random.permutation(jax.random.fold_in(own, 3), number_of)
    giver, taker = mixed[0:number_of // 2 * 2:2], mixed[1:number_of // 2 * 2:2]
    slack = jnp.minimum(tallies[giver] - 1, limit - tallies[taker]) // 2
    slack = jnp.where((giver == ranking[0]) | (taker == ranking[0]) | (tallies[taker] == 0), 0, jnp.maximum(slack, 0))
    passed = jax.random.randint(jax.random.fold_in(own, 4), (number_of // 2,), 0, 1 << 20) % (slack + 1)
    tallies = tallies.at[giver].add(-passed).at[taker].add(passed)
    members = jnp.searchsorted(jnp.cumsum(tallies), jnp.arange(rows * top), side="right").astype(jnp.int32)
    grid = members.reshape(top, rows).T
    grid = grid[jax.random.permutation(jax.random.fold_in(own, 1), rows)]
    offset_by = jax.random.randint(jax.random.fold_in(own, 2), (rows, 1), 0, top)
    return jnp.take_along_axis(grid, (jnp.arange(top)[None, :] + offset_by) % top, axis=1)


def portions_of(number_of, total, limit, skew, full):
    weights = [(1 << 20) // math.isqrt(grade ** skew) + 1 for grade in range(1, number_of + 1)]
    largest = limit if full else min(limit, max(-(-total // number_of), total * weights[0] // sum(weights)))
    least = 1 if total - largest >= number_of - 1 else 0
    counts, spare = [largest] + [least] * (number_of - 1), total - largest - least * (number_of - 1)
    while spare > 0:
        candidates = [i for i in range(1, number_of) if counts[i] < largest] or [i for i in range(1, number_of) if counts[i] < limit]
        whole, left = sum([weights[i] for i in candidates]), spare
        for i in candidates:
            more = min(limit - counts[i], max(1, left * weights[i] // whole), spare)
            counts[i] = counts[i] + more
            spare = spare - more
    return np.array(counts)


def gaussian(rng, shape, scale, reach, cuts=(), kind=jnp.bfloat16):
    drawn = scale * jax.random.normal(rng, shape, jnp.float32)
    if cuts:
        drawn = drawn * level_of(rng, shape, cuts, -0.22, 0.18)
    return jnp.clip(drawn, -reach, reach).astype(kind)


def setup_inputs(seed: int = 0) -> dict:
    splits = jax.random.split(jax.random.key(seed), 6)
    density = gaussian(splits[0], (NAUX, NOCC, NCABS), 1.0, 6.0, ((0, 32), (2, 16)))
    occ_density = gaussian(splits[1], (NAUX, NOCC, NOCC), 1.0, 6.0, ((0, 32),))
    cabs_coeff = gaussian(splits[2], (NAO, NCABS), NCABS ** -0.5, 0.0625, ((0, 32), (1, 16)))
    occ_coeff = gaussian(splits[3], (NAO, NOCC), NOCC ** -0.5, 0.5, ((0, 32),))
    tile_owner_keys = jax.random.split(jax.random.fold_in(splits[4], 1), NTILE // NTILE)
    tile_owner_turns = jax.random.permutation(jax.random.fold_in(splits[4], 3), NTILE // NTILE)
    tile_owner = jax.vmap(lambda own, number: shared_out(jax.random.fold_in(splits[4], 2), own, number, NTILE, N_SHELL, 1, CAPT, 2))(tile_owner_keys, tile_owner_turns).reshape((NTILE, 1))
    return {"density": density, "occ_density": occ_density, "cabs_coeff": cabs_coeff, "occ_coeff": occ_coeff, "tile_owner": tile_owner}


def reference(density, occ_density, cabs_coeff, occ_coeff, tile_owner):
    count = density.shape[0]
    flat = density.reshape(count * NOCC, NCABS)
    cshard = NCABS // N_SHELL

    def add_shard(total, shard):
        start = (shard * cshard).astype(jnp.int32)
        rows = lax.dynamic_slice_in_dim(flat, start, cshard, 1)
        cols = lax.dynamic_slice_in_dim(cabs_coeff, start, cshard, 1)
        part = lax.dot_general(rows, cols, (((1,), (1,)), ((), ())), preferred_element_type=jnp.float32)
        part = lax.optimization_barrier(part.astype(jnp.bfloat16))
        return total + part.astype(jnp.float32), None

    cabs, unused = lax.scan(add_shard, jnp.zeros((count * NOCC, NAO), jnp.float32), jnp.arange(N_SHELL, dtype=jnp.int32))
    occ_term = jnp.einsum("qij,nj->qin", occ_density.astype(jnp.float32), occ_coeff.astype(jnp.float32), precision=lax.Precision.HIGHEST)
    half = (cabs.reshape(count, NOCC, NAO) + occ_term).astype(jnp.bfloat16)
    blocks = half.astype(jnp.float32).reshape(count, NOCC, NTILE, BW)
    owners = tile_owner[:, 0]
    coeff = occ_coeff.astype(jnp.float32)

    def one_owner(owner):
        owned = (owners == owner).astype(jnp.int32)
        rank = jnp.cumsum(owned) - 1
        select = ((rank[None, :] == jnp.arange(CAPT, dtype=jnp.int32)[:, None]) & (owned[None, :] == 1)).astype(jnp.float32)
        picked = jnp.einsum("kt,qitw->kqiw", select, blocks, precision=lax.Precision.HIGHEST)
        result = jnp.einsum("kqiw,mi->kqwm", picked, coeff, precision=lax.Precision.HIGHEST)
        return result.astype(jnp.bfloat16)

    stacked = lax.map(one_owner, jnp.arange(N_SHELL, dtype=jnp.int32))
    return stacked.reshape(N_SHELL * CAPT, count, BW, NAO)
```

```python
import jax
import jax.numpy as jnp
from jax import lax
from jax.experimental import pallas as pl
from jax.experimental.pallas import tpu as pltpu
from jax.sharding import Mesh
from jax.sharding import PartitionSpec as P

AXES = ("y", "x", "c")
OFFSETS = (1, 3, 2)
ORDER = (0, 1, 3, 2)
NOCC, ZN, SLOTS, BW, TILES = 120, 16, 8, 32, 64
NQ, NG, GW, ST = 4, 4, 8, 4
LANES = 128
FAR = (8, 7, 9, 6, 10, 5, 11, 4, 12, 3, 13, 2, 14, 1, 15)
F32, BF16 = jnp.float32, jnp.bfloat16


def nt(a, b):
    return lax.dot_general(a, b, (((1,), (1,)), ((), ())), preferred_element_type=F32)


def exchange(
    dens, occd, cabs, occ, own_row, own_col, half_out, occ_out,
    xv, dv, cv, ga, gb, og, part, recv, send, sel, oterm, orow, asend, arecv,
    lsem, gs, gr, rs, rr, ts, tr,
):
    y, x, c, z = (lax.axis_index(a) for a in ("y", "x", "c", "z"))
    size = {"y": 4, "x": 4, "c": 2, "z": ZN}

    def at(axis, offset):
        return {axis: lax.rem(lax.axis_index(axis) + offset % size[axis], size[axis])}

    loads = [
        pltpu.make_async_copy(cabs, cv, lsem.at[0]),
        pltpu.make_async_copy(dens, xv, lsem.at[1]),
        pltpu.make_async_copy(occ, og.at[y, x, c], lsem.at[2]),
        pltpu.make_async_copy(occd, dv, lsem.at[3]),
    ]
    for load in loads:
        load.start()
    barrier = pltpu.get_barrier_semaphore()
    peers = [at(a, o) for a in ("x", "y") for o in OFFSETS] + [at("c", 1), at("z", 1), at("z", -1)]
    for peer in peers:
        pl.semaphore_signal(barrier, inc=1, device_id=peer, device_id_type=pl.DeviceIdType.MESH)

    count = [0]
    started = []

    def copy(src, dst, peer):
        k = count[0]
        count[0] += 1
        made = pltpu.make_async_remote_copy(
            src_ref=src, dst_ref=dst, send_sem=gs.at[k], recv_sem=gr.at[k],
            device_id=peer, device_id_type=pl.DeviceIdType.MESH,
        )
        made.start()
        started.append(made)
        return made

    loads[0].wait()
    mine = cv[...].astype(F32).reshape(2, NG, GW, cv.shape[1])
    ra = pl.multiple_of(c * 64 + x * 16, 16)
    rb = pl.multiple_of(c * 64 + y * 16, 16)
    for g in range(2):
        ga[y, g, pl.ds(ra, 16), :] = jnp.concatenate([mine[0, g], mine[1, g]], 0).astype(BF16)
        gb[x, g, pl.ds(rb, 16), :] = jnp.concatenate([mine[0, g + 2], mine[1, g + 2]], 0).astype(BF16)
    pl.semaphore_wait(barrier, len(peers))

    def blk_a(o):
        r = pl.multiple_of(c * 64 + lax.rem(x + 4 - o, 4) * 16, 16)
        return ga.at[y, :, pl.ds(r, 16), :]

    def blk_b(o):
        r = pl.multiple_of(c * 64 + lax.rem(y + 4 - o, 4) * 16, 16)
        return gb.at[x, :, pl.ds(r, 16), :]

    rc = pl.multiple_of(c * 64, 64)

    def qtr_a(o):
        return ga.at[lax.rem(y + 4 - o, 4), :, pl.ds(rc, 64), :]

    def qtr_b(o):
        return gb.at[lax.rem(x + 4 - o, 4), :, pl.ds(rc, 64), :]

    other = at("c", 1)
    a1 = [copy(blk_a(0), blk_a(0), at("x", o)) for o in OFFSETS]
    b1 = [copy(blk_b(0), blk_b(0), at("y", o)) for o in OFFSETS]
    fwd0 = [copy(blk_a(0), blk_a(0), other), copy(blk_b(0), blk_b(0), other)]
    for i, o in enumerate(OFFSETS):
        a1[i].wait_recv()
        fwd0.append(copy(blk_a(o), blk_a(o), other))
    a2 = [copy(qtr_a(0), qtr_a(0), at("y", o)) for o in OFFSETS]
    for i, o in enumerate(OFFSETS):
        b1[i].wait_recv()
        fwd0.append(copy(blk_b(o), blk_b(o), other))
    b2 = [copy(qtr_b(0), qtr_b(0), at("x", o)) for o in OFFSETS]
    loads[2].wait()
    o1 = [copy(og.at[y, x, c], og.at[y, x, c], at("x", o)) for o in OFFSETS]
    loads[1].wait()
    loads[3].wait()

    fwd = {}

    def forward(j):
        a2[j - 1].wait_recv()
        b2[j - 1].wait_recv()
        fwd[j] = (copy(qtr_a(ORDER[j]), qtr_a(ORDER[j]), other), copy(qtr_b(ORDER[j]), qtr_b(ORDER[j]), other))

    def compute(j):
        for made in fwd0 if j == 0 else fwd[j]:
            made.wait_recv()
        for base, ref in ((0, ga.at[lax.rem(y + 4 - ORDER[j], 4)]), (2, gb.at[lax.rem(x + 4 - ORDER[j], 4)])):
            got = nt(xv[...], ref[...].reshape(2 * LANES, xv.shape[1]))
            for q in range(NQ):
                for g in range(2):
                    part[j, q * NG + base + g] = got[q * NOCC:(q + 1) * NOCC, g * LANES:(g + 1) * LANES]

    def ring(way, s, j):
        return pltpu.make_async_remote_copy(
            src_ref=send.at[way, s, j], dst_ref=recv.at[way, s, j], send_sem=rs.at[way, s, j],
            recv_sem=rr.at[way, s, j], device_id=at("z", 1 if way == 0 else -1), device_id_type=pl.DeviceIdType.MESH,
        )

    def travels(way, s, j):
        return s >= 1 or way == j % 2

    def step(j, s):
        for way in range(2):
            if not travels(way, s, j):
                continue
            dest = lax.rem(z + (8 - s if way == 0 else 8 + s), ZN)
            value = part[j, dest]
            if s >= 1 and travels(way, s - 1, j):
                ring(way, s - 1, j).wait_recv()
                value = value + recv[way, s - 1, j].astype(F32)
            send[way, s, j] = value.astype(BF16)
            ring(way, s, j).start()

    q_me, g_me = z // NG, lax.rem(z, NG)

    def tile_of(stream, core, v, low):
        o = jnp.where(stream == 0, 0, jnp.where(stream == 1, 1, jnp.where(stream == 2, 3, 2)))
        ta = ((y + 4 - o) & 3) * 16 + v * 4
        tb = v * 16 + ((x + 4 - o) & 3) * 4
        return jnp.where(g_me < 2, ta, tb) + core * 2 + low

    def selection():
        row, col = own_row[...], own_col[...]
        before = lax.broadcasted_iota(jnp.int32, (TILES, TILES), 0) < lax.broadcasted_iota(jnp.int32, (TILES, TILES), 1)
        rank = jnp.sum(jnp.where(before & (col == row), 1.0, 0.0), axis=0, keepdims=True)
        slot = (row * SLOTS).astype(F32) + rank
        lane = lax.broadcasted_iota(jnp.int32, (TILES, ST * LANES), 1)
        tile = tile_of(lane >> 7, (lane >> 6) & 1, (lane >> 4) & 3, (lane >> 3) & 1)
        spread = jnp.where(tile == lax.broadcasted_iota(jnp.int32, (TILES, ST * LANES), 0), 1.0, 0.0).astype(BF16)
        lifted = lax.dot_general(
            jnp.broadcast_to(slot, (8, TILES)).astype(BF16), spread, (((1,), (0,)), ((), ())), preferred_element_type=F32
        )
        place = lifted[0:1].astype(jnp.int32) * GW + (lax.broadcasted_iota(jnp.int32, (1, ST * LANES), 1) & 7)
        for o in range(ZN):
            rows = lax.broadcasted_iota(jnp.int32, (64, ST * LANES), 0) + o * 64
            sel[o * 64:(o + 1) * 64, :] = jnp.where(rows == place, 1.0, 0.0).astype(BF16)

    fo, o2 = [], []

    def occ_second():
        for made in o1:
            made.wait_recv()
        o2.extend(copy(og.at[y, :, c], og.at[y, :, c], at("y", o)) for o in OFFSETS)
        fo.append(copy(og.at[y, :, c], og.at[y, :, c], other))

    def occ_third():
        for i, o in enumerate(OFFSETS):
            o2[i].wait_recv()
            yy = lax.rem(y + 4 - o, 4)
            fo.append(copy(og.at[yy, :, c], og.at[yy, :, c], other))

    def occ_last():
        for made in fo:
            made.wait_recv()
        occ_out[...] = og[...]

    def occ_term():
        for j in range(ST):
            for r in range(16):
                core, v, low = r // 8, (r // 2) % 4, r % 2
                t = tile_of(j, core, v, low)
                got = og[t // 16, (t // 4) & 3, core, low * NG + g_me]
                orow[(j * 16 + r) * GW:(j * 16 + r + 1) * GW, :] = got.astype(F32)
        oterm[...] = nt(dv[q_me], orow[...].astype(BF16))

    compute(0)
    step(0, 0)
    step(0, 1)
    forward(1)
    forward(2)
    compute(1)
    step(1, 0)
    compute(2)
    step(2, 0)
    step(0, 2)
    forward(3)
    step(1, 1)
    step(2, 1)
    step(0, 3)
    compute(3)
    step(3, 0)
    occ_second()
    at_step = [4, 2, 2, 1]
    side = [selection, occ_third, occ_last, occ_term]
    while min(at_step) < 8:
        for j in range(ST):
            if at_step[j] < 8:
                step(j, at_step[j])
                at_step[j] += 1
        if side:
            side.pop(0)()

    total = []
    for j in range(ST):
        value = part[j, z] + oterm[:, j * LANES:(j + 1) * LANES]
        for way in range(2):
            ring(way, 7, j).wait_recv()
            value = value + recv[way, 7, j].astype(F32)
        total.append(value.astype(BF16))
    half = jnp.concatenate(total, axis=1)
    picked = lax.dot_general(sel[...], half, (((1,), (1,)), ((), ())), preferred_element_type=F32)
    asend[...] = picked.reshape(ZN, SLOTS, GW, NOCC).astype(BF16)

    def route(k):
        to = lax.rem(z + k, ZN)
        return pltpu.make_async_remote_copy(
            src_ref=asend.at[to], dst_ref=arecv.at[z], send_sem=ts.at[k], recv_sem=tr.at[k],
            device_id={"z": to}, device_id_type=pl.DeviceIdType.MESH,
        )

    for k in FAR:
        route(k).start()
    arecv[z] = asend[z]
    for made in started:
        made.wait_send()
    for way in range(2):
        for s in range(8):
            for j in range(ST):
                if travels(way, s, j):
                    ring(way, s, j).wait_send()
    for k in FAR:
        route(k).wait_recv()
    half_out[...] = arecv[...]
    for k in FAR:
        route(k).wait_send()


def final(half, occ, out):
    rows = half[...].astype(F32)
    kk = rows.shape[1]
    lhs = jnp.concatenate([rows[:, k].reshape(LANES, NOCC) for k in range(kk)], axis=0).astype(BF16)
    got = nt(lhs, occ[...])
    out[...] = got.reshape(kk, NQ, BW, got.shape[1]).astype(BF16)


def per_device(density, occ_density, cabs_coeff, occ_coeff, tile_owner):
    nq, nocc, ncab = density.shape
    rows = nq * nocc
    nao = TILES * BW
    any_spec = pl.BlockSpec(memory_space=pl.ANY)
    vmem = pl.BlockSpec(memory_space=pltpu.VMEM)
    half, occ_full = pl.pallas_call(
        exchange,
        out_shape=(
            jax.ShapeDtypeStruct((ZN, SLOTS, GW, nocc), BF16),
            jax.ShapeDtypeStruct((4, 4, 2, 8, GW, nocc), BF16),
        ),
        in_specs=[any_spec] * 4 + [vmem] * 2,
        out_specs=(vmem, vmem),
        scratch_shapes=[
            pltpu.VMEM((rows, ncab), BF16),
            pltpu.VMEM((nq, nocc, nocc), BF16),
            pltpu.VMEM((64, ncab), BF16),
            pltpu.VMEM((4, 2, LANES, ncab), BF16),
            pltpu.VMEM((4, 2, LANES, ncab), BF16),
            pltpu.VMEM((4, 4, 2, 8, GW, nocc), BF16),
            pltpu.VMEM((ST, ZN, nocc, LANES), F32),
            pltpu.VMEM((2, 8, ST, nocc, LANES), BF16),
            pltpu.VMEM((2, 8, ST, nocc, LANES), BF16),
            pltpu.VMEM((ZN * SLOTS * GW, ST * LANES), BF16),
            pltpu.VMEM((nocc, ST * LANES), F32),
            pltpu.VMEM((ST * LANES, nocc), F32),
            pltpu.VMEM((ZN, SLOTS, GW, nocc), BF16),
            pltpu.VMEM((ZN, SLOTS, GW, nocc), BF16),
            pltpu.SemaphoreType.DMA((4,)),
            pltpu.SemaphoreType.DMA((36,)),
            pltpu.SemaphoreType.DMA((36,)),
            pltpu.SemaphoreType.DMA((2, 8, ST)),
            pltpu.SemaphoreType.DMA((2, 8, ST)),
            pltpu.SemaphoreType.DMA((ZN,)),
            pltpu.SemaphoreType.DMA((ZN,)),
        ],
        compiler_params=pltpu.CompilerParams(
            collective_id=0, has_side_effects=True, vmem_limit_bytes=40 * 1024 * 1024
        ),
    )(
        density.reshape(rows, ncab),
        occ_density,
        cabs_coeff,
        occ_coeff.reshape(8, GW, nocc),
        tile_owner.reshape(1, TILES),
        tile_owner,
    )
    steps = 4
    per = SLOTS // steps
    return pl.pallas_call(
        final,
        grid=(steps,),
        out_shape=jax.ShapeDtypeStruct((SLOTS, nq, BW, nao), BF16),
        in_specs=[
            pl.BlockSpec((ZN, per, GW, nocc), lambda k: (0, k, 0, 0)),
            pl.BlockSpec((nao, nocc), lambda k: (0, 0)),
        ],
        out_specs=pl.BlockSpec((per, nq, BW, nao), lambda k: (k, 0, 0, 0)),
    )(half, occ_full.reshape(nao, nocc))


def solution(mesh):
    split = Mesh(mesh.devices.reshape(4, 4, 2, mesh.shape["shell"]), (*AXES, "z"))
    placed = (P(AXES, None, "z"), P(AXES, None, None), P(AXES, "z"), P(AXES, None), P())
    return jax.shard_map(
        per_device, mesh=split, in_specs=placed, out_specs=P("z", AXES, None, None), check_vma=False
    )
```
